32 devices in a mesh: dp: 1 (over z), tp: 4 (over y), ep: 8 (over x, core).
Axes of the slice: x: 4, y: 4, z: 1, core: 2. Of those that a mesh axis runs over, the one named last changes fastest.
The devices are a block of a 4x4x8 slice.
Arguments:
- act_in: bfloat16 [131072, 768], P(('dp', 'ep'))
- expert_idx: int32 [131072, 1], P(('dp', 'ep'))
- gate_vals: float32 [131072, 1], P(('dp', 'ep'))
- w_in: bfloat16 [16, 768, 3072], P('ep', None, 'tp')
- w_out: bfloat16 [16, 3072, 768], P('ep', 'tp')
Outputs:
- output: bfloat16 [131072, 768], P(('dp', 'ep'))
All inputs are finite; a program needn't handle non-finite values.
Results may differ from the reference program's by a relative error of at most 0.001.
Values are sent between devices in bfloat16 or wider.
A program may use at most 768 MiB of HBM per device.

```python
import jax
import jax.numpy as jnp
from jax import lax

SOURCES = 8
TOKENS_DEV = 16384
HIDDEN = 768
FF_DIM = 3072
EXPERTS = 16
TOP_K = 1
CAPACITY = 1280
NUM_TOK = SOURCES * TOKENS_DEV
NUM_SLOTS = EXPERTS * SOURCES * CAPACITY


def draw_routing(rng_key):
    key_first, key_gap, key_hot = jax.random.split(rng_key, 3)
    first_ids = jax.random.randint(key_first, (SOURCES, TOKENS_DEV), 0, EXPERTS, jnp.int32)
    hot_ids = jax.random.randint(key_hot, (SOURCES, 1), 0, EXPERTS, jnp.int32)
    forced = jnp.arange(TOKENS_DEV)[None, :] < CAPACITY + 8
    first_ids = jnp.where(forced, hot_ids, first_ids)
    gap_sizes = jax.random.randint(key_gap, (SOURCES, TOKENS_DEV, TOP_K - 1), 1, EXPERTS // TOP_K + 1, jnp.int32)
    offsets = jnp.concatenate([jnp.zeros((SOURCES, TOKENS_DEV, 1), jnp.int32), jnp.cumsum(gap_sizes, axis=2)], axis=2)
    return ((first_ids[:, :, None] + offsets) % EXPERTS).reshape(NUM_TOK, TOP_K).astype(jnp.int32)


def setup_inputs(seed: int = 0, part: int = 0) -> dict:
    weight_keys = jax.random.split(jax.random.key(seed), 2)
    w_in = (jax.random.normal(weight_keys[0], (EXPERTS, HIDDEN, FF_DIM), jnp.float32) * HIDDEN ** -0.5).astype(jnp.bfloat16)
    w_out = (jax.random.normal(weight_keys[1], (EXPERTS, FF_DIM, HIDDEN), jnp.float32) * FF_DIM ** -0.5).astype(jnp.bfloat16)
    part_keys = jax.random.split(jax.random.fold_in(jax.random.key(seed + 1), part), 3)
    act_in = jax.random.normal(part_keys[0], (NUM_TOK, HIDDEN), jnp.float32).astype(jnp.bfloat16)
    expert_idx = draw_routing(part_keys[1])
    gate_vals = jax.random.uniform(part_keys[2], (NUM_TOK, TOP_K), jnp.float32, 0.5, 1.5) * TOP_K ** -0.5
    return {"act_in": act_in, "expert_idx": expert_idx, "gate_vals": gate_vals, "w_in": w_in, "w_out": w_out}


def slot_ids_of(src_idx):
    hit_mask = src_idx[:, :, :, None] == jnp.arange(EXPERTS)
    per_tok = jnp.sum(hit_mask, axis=2, dtype=jnp.int32)
    preceding = jnp.cumsum(per_tok, axis=1) - per_tok
    return jnp.sum(jnp.where(hit_mask, preceding[:, :, None, :], 0), axis=3)


def reference(act_in, expert_idx, gate_vals, w_in, w_out):
    src_idx = expert_idx.reshape(SOURCES, TOKENS_DEV, TOP_K)
    slot_ids = slot_ids_of(src_idx)
    src_ids = jnp.arange(SOURCES)[:, None, None]
    slot_pos = jnp.where(slot_ids < CAPACITY, (src_idx * SOURCES + src_ids) * CAPACITY + slot_ids, NUM_SLOTS).reshape(-1)
    tok_ids = jnp.broadcast_to(src_ids * TOKENS_DEV + jnp.arange(TOKENS_DEV)[None, :, None], src_idx.shape).reshape(-1)
    tok_table = jnp.full((NUM_SLOTS + 1,), NUM_TOK, jnp.int32).at[slot_pos].set(tok_ids)[:NUM_SLOTS]
    gate_table = jnp.zeros((NUM_SLOTS + 1,), jnp.float32).at[slot_pos].set(gate_vals.reshape(-1))[:NUM_SLOTS]
    padded = jnp.concatenate([act_in, jnp.zeros((1, HIDDEN), act_in.dtype)], axis=0)

    def one_expert(acc_rows, packed):
        w_first, w_second, tok_rows, gate_rows = packed
        expert_rows = padded[tok_rows]
        pre_act = jnp.dot(expert_rows, w_first, preferred_element_type=jnp.float32)
        hidden_act = jax.nn.gelu(pre_act, approximate=True).astype(jnp.bfloat16)
        expert_out = jnp.dot(hidden_act, w_second, preferred_element_type=jnp.float32).astype(jnp.bfloat16)
        acc_rows = acc_rows.at[tok_rows].add(gate_rows[:, None] * expert_out.astype(jnp.float32))
        return acc_rows, None

    packed_all = (w_in, w_out, tok_table.reshape(EXPERTS, SOURCES * CAPACITY), gate_table.reshape(EXPERTS, SOURCES * CAPACITY))
    summed_rows = lax.scan(one_expert, jnp.zeros((NUM_TOK + 1, HIDDEN), jnp.float32), packed_all)[0]
    return summed_rows[:NUM_TOK].astype(jnp.bfloat16)
```

```python
import functools

import jax
import jax.numpy as jnp
from jax import lax
from jax.experimental import pallas as pl
from jax.experimental.pallas import tpu as pltpu
from jax.sharding import PartitionSpec as P

LANES = 128
WIN = 16
BLOCK = 256
ROW_TILE = 256
COL_SPAN = 1024
SHARES = (2, 5, 8, 5)


def capacity_of(top_k, tokens, experts, tp_size):
    divisor = 32 * experts * tp_size
    return 8 * tp_size * ((5 * top_k * tokens + divisor - 1) // divisor)


def tri(n, inclusive):
    rows = lax.broadcasted_iota(jnp.int32, (n, n), 0)
    cols = lax.broadcasted_iota(jnp.int32, (n, n), 1)
    return (rows <= cols if inclusive else rows < cols).astype(jnp.bfloat16)


def int_dot(spec, a, b):
    return jnp.einsum(spec, a.astype(jnp.bfloat16), b.astype(jnp.bfloat16), preferred_element_type=jnp.float32)


def ffn_kernel(x_ref, *refs):
    w_refs, out_ref = refs[:8], refs[-1]
    x = x_ref[...]
    total = None
    for shard in range(4):
        pre = jnp.dot(x, w_refs[shard][...], preferred_element_type=jnp.float32)
        act = jax.nn.gelu(pre, approximate=True).astype(jnp.bfloat16)
        part = jnp.dot(act, w_refs[4 + shard][...], preferred_element_type=jnp.float32)
        total = part if total is None else total + part
    out_ref[...] = total.astype(out_ref.dtype)


def ffn(x, w_ins, w_outs, after):
    rows, hidden = x.shape
    width = w_ins[0].shape[1]
    fixed = lambda i: (0, 0)
    specs = [pl.BlockSpec((ROW_TILE, hidden), lambda i: (i, 0))]
    specs += [pl.BlockSpec((hidden, width), fixed)] * 4 + [pl.BlockSpec((width, hidden), fixed)] * 4
    specs += [pl.BlockSpec(memory_space=pl.ANY)] * len(after)
    return pl.pallas_call(
        ffn_kernel,
        grid=(rows // ROW_TILE,),
        in_specs=specs,
        out_specs=pl.BlockSpec((ROW_TILE, hidden), lambda i: (i, 0)),
        out_shape=jax.ShapeDtypeStruct((rows, hidden), jnp.bfloat16),
        compiler_params=pltpu.CompilerParams(dimension_semantics=("arbitrary",), vmem_limit_bytes=60 * 2**20),
        cost_estimate=pl.CostEstimate(flops=16 * rows * hidden * width, bytes_accessed=4 * rows * hidden + 16 * hidden * width, transcendentals=4 * rows * width),
        name="ffn",
    )(x, *w_ins, *w_outs, *after)


def combine_kernel(chunk, active_ref, count_ref, src_ref, table, col_ref, gate_ref, *refs):
    first = chunk == 0
    old_hbm, refs = (None, refs) if first else (refs[0], refs[1:])
    out_hbm, held, old_buf, out_buf, acc, win_sem, old_sem, out_sem = refs
    steps = count_ref.shape[0]
    n_active = active_ref[steps]

    def rows_of(block):
        return pl.ds(pl.multiple_of(block * BLOCK, BLOCK), BLOCK)

    def window(block, slot, w):
        row = pl.multiple_of(src_ref[block, w] * WIN, WIN)
        return pltpu.make_async_copy(table.at[pl.ds(row, WIN), :], held.at[slot, pl.ds(pl.multiple_of(w * WIN, WIN), WIN), :], win_sem.at[slot, w])

    def earlier(block, slot):
        return pltpu.make_async_copy(old_hbm.at[rows_of(block), :], old_buf.at[slot], old_sem.at[slot])

    def output(block, slot):
        return pltpu.make_async_copy(out_buf.at[slot], out_hbm.at[rows_of(block), :], out_sem.at[slot])

    def fetch(i, slot):
        block = active_ref[i]
        if not first:
            earlier(block, slot).start()

        def issue(w, _):
            window(block, slot, w).start()
            return 0

        lax.fori_loop(0, count_ref[block], issue, 0)

    held[...] = jnp.zeros_like(held)

    @pl.when(n_active > 0)
    def _():
        fetch(0, 0)

    def body(i, _):
        slot = i % 2
        block = active_ref[i]

        @pl.when(i + 1 < n_active)
        def _():
            fetch(i + 1, 1 - slot)

        if not first:
            earlier(block, slot).wait()
        n = count_ref[block]

        def land(w, _):
            window(block, slot, w).wait()
            return 0

        lax.fori_loop(0, n, land, 0)

        @pl.when(i >= 2)
        def _():
            output(active_ref[i - 2], slot).wait()

        def down(ref):
            return jnp.broadcast_to(ref[pl.ds(block, 1), :], (LANES, BLOCK)).T

        depth = 2 * LANES
        lane = lax.broadcasted_iota(jnp.int32, (BLOCK, LANES), 1).astype(jnp.float32)
        col = down(col_ref) - chunk * COL_SPAN - lane

        def part(k):
            at = lax.convert_element_type(k * depth, jnp.float32)
            pick = jnp.concatenate([(col == at + LANES * j).astype(jnp.float32).astype(jnp.bfloat16) for j in range(2)], axis=1)
            return jnp.dot(pick, held[slot, pl.ds(pl.multiple_of(k * depth, depth), depth), :], preferred_element_type=jnp.float32)

        acc[...] = part(0)

        def more(k, _):
            acc[...] += part(k)
            return 0

        lax.fori_loop(1, (n * WIN + depth - 1) // depth, more, 0)
        gate = down(gate_ref)
        for k in range(acc.shape[1] // LANES):
            cut = slice(k * LANES, (k + 1) * LANES)
            new = acc[:, cut] * gate
            if not first:
                new = new + old_buf[slot, :, cut].astype(jnp.float32)
            out_buf[slot, :, cut] = new.astype(out_buf.dtype)
        output(block, slot).start()
        return 0

    lax.fori_loop(0, n_active, body, 0)

    @pl.when(n_active > 1)
    def _():
        output(active_ref[n_active - 2], n_active % 2).wait()

    @pl.when(n_active > 0)
    def _():
        output(active_ref[n_active - 1], (n_active - 1) % 2).wait()


def combine(chunk, n_win, active, count, src, table, col, gate, old):
    tokens, hidden = col.size, table.shape[1]
    smem, any_ = pl.BlockSpec(memory_space=pltpu.SMEM), pl.BlockSpec(memory_space=pl.ANY)
    olds = [] if old is None else [old]
    block = lambda width, dtype: pltpu.VMEM((2, BLOCK, width), dtype)
    return pl.pallas_call(
        functools.partial(combine_kernel, chunk),
        in_specs=[smem] * 3 + [any_] + [pl.BlockSpec(memory_space=pltpu.VMEM)] * 2 + [any_] * len(olds),
        out_specs=any_,
        out_shape=jax.ShapeDtypeStruct((tokens, hidden), jnp.bfloat16),
        input_output_aliases={6: 0} if olds else {},
        scratch_shapes=[
            pltpu.VMEM((2, n_win * WIN, hidden), jnp.bfloat16),
            block(hidden, jnp.bfloat16),
            block(hidden, jnp.bfloat16),
            pltpu.VMEM((BLOCK, hidden), jnp.float32),
            pltpu.SemaphoreType.DMA((2, n_win)),
            pltpu.SemaphoreType.DMA((2,)),
            pltpu.SemaphoreType.DMA((2,)),
        ],
        compiler_params=pltpu.CompilerParams(vmem_limit_bytes=60 * 2**20),
        cost_estimate=pl.CostEstimate(flops=tokens * n_win * WIN * hidden, bytes_accessed=2 * tokens * hidden, transcendentals=0),
        name="combine",
    )(active, count, src, table, col, gate, *olds)


def solution(mesh):
    tp_size = mesh.shape["tp"]
    ep_size = mesh.shape["ep"]
    assert tp_size == 4

    def whole_moe(act_loc, idx_loc, gate_loc, w_in, w_out):
        tokens, hidden = act_loc.shape
        local_experts = w_in.shape[0]
        assert idx_loc.shape[1] == 1 and local_experts == 2
        experts = local_experts * ep_size
        capacity = capacity_of(1, tokens, experts, tp_size)
        shares = tp_size // local_experts
        chunks = len(SHARES)
        pieces = [capacity // shares * n // sum(SHARES) for n in SHARES]
        heads = [shares * sum(pieces[:q]) for q in range(chunks)]
        assert shares * sum(pieces) == capacity and all(ep_size * p % ROW_TILE == 0 and p % WIN == 0 for p in pieces)
        assert tokens % BLOCK == 0 and BLOCK % LANES == 0
        rank = lax.axis_index("tp")
        which = rank // shares

        twin = [(i, i ^ 1) for i in range(tp_size)]
        mirror = [(i, tp_size - 1 - i) for i in range(tp_size)]
        w_ins, w_outs = [], []
        for whole, kept in ((w_in, w_ins), (w_out, w_outs)):
            mine = lax.dynamic_index_in_dim(whole, which, 0, keepdims=False)
            other = lax.dynamic_index_in_dim(whole, 1 - which, 0, keepdims=False)
            across = lax.ppermute(other, "tp", mirror)
            near = lax.ppermute(mine, "tp", twin)
            far = lax.ppermute(across, "tp", twin)
            kept += [mine, near, across, far]

        blocks = tokens // LANES
        chosen = idx_loc.reshape(blocks, LANES)
        hits = chosen[None] == jnp.arange(experts, dtype=jnp.int32)[:, None, None]
        within = int_dot("ebi,ij->ebj", hits, tri(LANES, True))
        totals = within[:, :, LANES - 1]
        base = int_dot("eb,bc->ec", totals, tri(blocks, False))
        upto = base + totals
        slot = jnp.sum(jnp.where(hits, base[:, :, None] + within - 1, 0.0), axis=0).astype(jnp.int32)

        mine_of = lambda a: lax.dynamic_index_in_dim(a.reshape((ep_size, local_experts) + a.shape[1:]), which, 1, keepdims=False)
        my_within, my_base, my_upto = mine_of(within), mine_of(base), mine_of(upto)
        my_slot = jnp.concatenate([heads[q] + (rank % shares) * pieces[q] + jnp.arange(pieces[q], dtype=jnp.int32) for q in range(chunks)])
        my_slot = my_slot.astype(jnp.float32)
        in_block = jnp.sum((my_upto[:, None, :] <= my_slot[None, :, None]).astype(jnp.int32), axis=2)
        is_block = in_block[:, :, None] == jnp.arange(blocks, dtype=jnp.int32)
        row_within = int_dot("dsb,dbi->dsi", is_block, my_within)
        row_base = jnp.sum(jnp.where(is_block, my_base[:, None, :], 0.0), axis=2)
        in_row = jnp.sum((row_within <= (my_slot[None, :] - row_base)[:, :, None]).astype(jnp.int32), axis=2)
        tok = jnp.where(in_block < blocks, in_block * LANES + in_row, tokens)

        n_win = -(-(BLOCK + experts * 2 * (WIN - 1)) // WIN)
        n_win = -(-n_win * WIN // LANES) * LANES // WIN
        steps = tokens // BLOCK
        first = jnp.minimum(base[:, :: BLOCK // LANES], capacity).astype(jnp.int32).T
        last = jnp.minimum(upto[:, BLOCK // LANES - 1 :: BLOCK // LANES], capacity).astype(jnp.int32).T
        win_lo = first // WIN
        win_hi = jnp.where(last > first, (last - 1) // WIN + 1, win_lo)
        of_slot = lambda per_chunk, at: sum((per_chunk[q] - per_chunk[q - 1]) * (at >= heads[q]).astype(jnp.int32) if q else per_chunk[0] for q in range(chunks))
        edge = jnp.asarray([h // WIN for h in heads] + [capacity // WIN], jnp.int32)
        lo = jnp.maximum(win_lo[:, None, :], edge[None, :-1, None])
        count = jnp.maximum(jnp.minimum(win_hi[:, None, :], edge[None, 1:, None]) - lo, 0)
        ends = int_dot("sqe,ef->sqf", count, tri(experts, True)).astype(jnp.int32)
        starts = ends - count
        n_fetch = ends[:, :, experts - 1].T
        w_id = jnp.arange(n_win, dtype=jnp.int32)
        of_expert = jnp.sum((ends[:, :, None, :] <= w_id[None, None, :, None]).astype(jnp.int32), axis=3)
        is_expert = of_expert[:, :, :, None] == jnp.arange(experts, dtype=jnp.int32)
        win = jnp.sum(jnp.where(is_expert, (lo - starts)[:, :, None, :], 0), axis=3) + w_id - edge[None, :-1, None]
        per_piece = jnp.asarray([p // WIN for p in pieces], jnp.int32)[None, :, None]
        share_of = (win >= per_piece).astype(jnp.int32) if shares == 2 else win // per_piece
        of_rank = (of_expert % local_experts) * shares + share_of
        src = (of_rank * ep_size + of_expert // local_experts) * per_piece + win - share_of * per_piece
        src = jnp.where(of_expert < experts, src, 0)
        busy = (n_fetch > 0) | (jnp.arange(chunks)[:, None] == 0)
        before = int_dot("qs,st->qt", busy, tri(steps, True)).astype(jnp.int32)
        nth = jnp.arange(steps + 1, dtype=jnp.int32)
        active = jnp.sum((before[:, None, :] <= nth[None, :, None]).astype(jnp.int32), axis=2)
        active = jnp.where(nth[None] == steps, before[:, -1:], active)
        slot_rows = slot.reshape(steps, BLOCK)
        pair_of = of_slot([q * experts for q in range(chunks)], slot_rows) + idx_loc.reshape(steps, BLOCK)
        pairs = chunks * experts
        move = ((starts - lo) * WIN + jnp.arange(chunks, dtype=jnp.int32)[None, :, None] * COL_SPAN).reshape(steps, 1, pairs)
        shift = jnp.sum(jnp.where(pair_of[:, :, None] == jnp.arange(pairs, dtype=jnp.int32), move, 0), axis=2)
        col = jnp.where(slot_rows < capacity, slot_rows + shift, -1).astype(jnp.float32)
        gate = gate_loc.reshape(steps, BLOCK)

        def exchange(rows):
            return lax.all_to_all(rows.reshape(ep_size, -1, hidden), "ep", 0, 0, tiled=True)

        outgoing = []
        for q in range(chunks):
            at = sum(pieces[:q])
            rows = tok[:, at : at + pieces[q]].reshape(-1)
            outgoing.append(jnp.take(act_loc, rows, axis=0, mode="fill", fill_value=0))
        arrived = [exchange(outgoing[q]) for q in range(chunks - 1)]
        made, returned = [], []
        for q in range(chunks):
            if q == chunks - 1:
                outgoing[q], returned[q - 1] = lax.optimization_barrier((outgoing[q], returned[q - 1]))
                arrived.append(exchange(outgoing[q]))
            made.append(ffn(arrived[q].reshape(-1, hidden), w_ins, w_outs, made[q - 1 : q] if q else [outgoing[chunks - 1], arrived[1]]))
            if q == chunks - 1:
                made[q], col, gate, src, n_fetch, active = lax.optimization_barrier((made[q], col, gate, src, n_fetch, active))
            returned.append(exchange(made[q]))
        tables = [lax.all_gather(r, "tp", axis=0).reshape(-1, hidden) for r in returned]
        out = None
        for q in range(chunks):
            out = combine(q, n_win, active[q], n_fetch[q], src[:, q, :], tables[q], col, gate, out)
        return out

    tok_spec = P(("dp", "ep"), None)
    return jax.shard_map(whole_moe, mesh=mesh, in_specs=(tok_spec, tok_spec, tok_spec, P("ep", None, "tp"), P("ep", "tp", None)), out_specs=tok_spec, check_vma=False)
```

```python
import functools

import jax
import jax.numpy as jnp
from jax import lax
from jax.experimental import pallas as pl
from jax.experimental.pallas import tpu as pltpu
from jax.sharding import PartitionSpec as P

LANES = 128
WIN = 16
BLOCK = 256
ROW_TILE = 256
DEPTH = 512
COL_SPAN = 1024
SHARES = (2, 4, 5, 5, 4)


def capacity_of(top_k, tokens, experts, tp_size):
    divisor = 32 * experts * tp_size
    return 8 * tp_size * ((5 * top_k * tokens + divisor - 1) // divisor)


def tri(n, inclusive):
    rows = lax.broadcasted_iota(jnp.int32, (n, n), 0)
    cols = lax.broadcasted_iota(jnp.int32, (n, n), 1)
    return (rows <= cols if inclusive else rows < cols).astype(jnp.bfloat16)


def int_dot(spec, a, b):
    return jnp.einsum(spec, a.astype(jnp.bfloat16), b.astype(jnp.bfloat16), preferred_element_type=jnp.float32)


def ffn_kernel(x_ref, *refs):
    w_refs, out_ref = refs[:8], refs[-1]
    x = x_ref[...]
    total = None
    for shard in range(4):
        pre = jnp.dot(x, w_refs[shard][...], preferred_element_type=jnp.float32)
        act = jax.nn.gelu(pre, approximate=True).astype(jnp.bfloat16)
        part = jnp.dot(act, w_refs[4 + shard][...], preferred_element_type=jnp.float32)
        total = part if total is None else total + part
    out_ref[...] = total.astype(out_ref.dtype)


def ffn(x, w_ins, w_outs, after):
    rows, hidden = x.shape
    width = w_ins[0].shape[1]
    fixed = lambda i: (0, 0)
    specs = [pl.BlockSpec((ROW_TILE, hidden), lambda i: (i, 0))]
    specs += [pl.BlockSpec((hidden, width), fixed)] * 4 + [pl.BlockSpec((width, hidden), fixed)] * 4
    specs += [pl.BlockSpec(memory_space=pl.ANY)] * len(after)
    return pl.pallas_call(
        ffn_kernel,
        grid=(rows // ROW_TILE,),
        in_specs=specs,
        out_specs=pl.BlockSpec((ROW_TILE, hidden), lambda i: (i, 0)),
        out_shape=jax.ShapeDtypeStruct((rows, hidden), jnp.bfloat16),
        compiler_params=pltpu.CompilerParams(dimension_semantics=("arbitrary",), vmem_limit_bytes=60 * 2**20),
        cost_estimate=pl.CostEstimate(flops=16 * rows * hidden * width, bytes_accessed=4 * rows * hidden + 16 * hidden * width, transcendentals=4 * rows * width),
        name="ffn",
    )(x, *w_ins, *w_outs, *after)


def combine_kernel(chunk, n_win, n_tables, active_ref, bound_ref, src_ref, *refs):
    tables, (col_ref, gate_ref), refs = refs[:n_tables], refs[n_tables : n_tables + 2], refs[n_tables + 2 :]
    first = chunk == 0
    old_hbm, refs = (None, refs) if first else (refs[0], refs[1:])
    out_hbm, held, old_buf, out_buf, win_sem, old_sem, out_sem, nil_sem = refs
    steps = bound_ref.shape[0]
    n_active = active_ref[steps]

    def rows_of(block):
        return pl.ds(pl.multiple_of(block * BLOCK, BLOCK), BLOCK)

    def window(table, block, slot, w):
        row = pl.multiple_of(src_ref[block, w] * WIN, WIN)
        return pltpu.make_async_copy(table.at[pl.ds(row, WIN), :], held.at[slot, pl.ds(pl.multiple_of(w * WIN, WIN), WIN), :], win_sem.at[slot, w])

    def earlier(block, slot):
        return pltpu.make_async_copy(old_hbm.at[rows_of(block), :], old_buf.at[slot], old_sem.at[slot])

    def output(block, slot):
        return pltpu.make_async_copy(out_buf.at[slot], out_hbm.at[rows_of(block), :], out_sem.at[slot])

    def fetch(i, slot):
        block = active_ref[i]
        if not first:
            earlier(block, slot).start()

        for k, table in enumerate(tables):

            def issue(w, _, table=table):
                window(table, block, slot, w).start()
                return 0

            lax.fori_loop(bound_ref[block, k], bound_ref[block, k + 1], issue, 0)

    def nil(block):
        return pltpu.make_async_copy(old_buf.at[0], out_hbm.at[rows_of(block), :], nil_sem.at[block])

    def clear(block, _):
        @pl.when(bound_ref[block, n_tables] == 0)
        def _():
            nil(block).start()

        return 0

    def cleared(block, _):
        @pl.when(bound_ref[block, n_tables] == 0)
        def _():
            nil(block).wait()

        return 0

    held[...] = jnp.zeros_like(held)
    if first:
        old_buf[0] = jnp.zeros(old_buf.shape[1:], old_buf.dtype)
        lax.fori_loop(0, steps, clear, 0)

    @pl.when(n_active > 0)
    def _():
        fetch(0, 0)

    def body(i, _):
        slot = i % 2
        block = active_ref[i]

        @pl.when(i + 1 < n_active)
        def _():
            fetch(i + 1, 1 - slot)

        if not first:
            earlier(block, slot).wait()
        n = bound_ref[block, n_tables]

        def land(w, _):
            window(tables[0], block, slot, w).wait()
            return 0

        lax.fori_loop(0, n, land, 0)

        @pl.when(i >= 2)
        def _():
            output(active_ref[i - 2], slot).wait()

        def down(ref):
            return jnp.broadcast_to(ref[pl.ds(block, 1), :], (LANES, BLOCK)).T

        def gathered(depth):
            lane = lax.broadcasted_iota(jnp.int32, (BLOCK, LANES), 1).astype(jnp.float32)
            col = down(col_ref) - chunk * COL_SPAN - lane
            gate = down(gate_ref)
            pick = jnp.concatenate([(col == LANES * j).astype(jnp.float32).astype(jnp.bfloat16) for j in range(depth // LANES)], axis=1)
            rows = jnp.dot(pick, held[slot, :depth, :], preferred_element_type=jnp.float32)
            for k in range(rows.shape[1] // LANES):
                cut = slice(k * LANES, (k + 1) * LANES)
                new = rows[:, cut] * gate
                if not first:
                    new = new + old_buf[slot, :, cut].astype(jnp.float32)
                out_buf[slot, :, cut] = new.astype(out_buf.dtype)

        @pl.when(n <= DEPTH // WIN)
        def _():
            gathered(DEPTH)

        @pl.when(n > DEPTH // WIN)
        def _():
            gathered(n_win * WIN)

        output(block, slot).start()
        return 0

    lax.fori_loop(0, n_active, body, 0)
    if first:
        lax.fori_loop(0, steps, cleared, 0)

    @pl.when(n_active > 1)
    def _():
        output(active_ref[n_active - 2], n_active % 2).wait()

    @pl.when(n_active > 0)
    def _():
        output(active_ref[n_active - 1], (n_active - 1) % 2).wait()


def combine(chunk, n_win, active, bound, src, tables, col, gate, old):
    tokens, hidden = col.size, tables[0].shape[1]
    smem, any_ = pl.BlockSpec(memory_space=pltpu.SMEM), pl.BlockSpec(memory_space=pl.ANY)
    olds = [] if old is None else [old]
    block = lambda width, dtype: pltpu.VMEM((2, BLOCK, width), dtype)
    return pl.pallas_call(
        functools.partial(combine_kernel, chunk, n_win, len(tables)),
        in_specs=[smem] * 3 + [any_] * len(tables) + [pl.BlockSpec(memory_space=pltpu.VMEM)] * 2 + [any_] * len(olds),
        out_specs=any_,
        out_shape=jax.ShapeDtypeStruct((tokens, hidden), jnp.bfloat16),
        input_output_aliases={5 + len(tables): 0} if olds else {},
        scratch_shapes=[
            pltpu.VMEM((2, n_win * WIN, hidden), jnp.bfloat16),
            block(hidden, jnp.bfloat16),
            block(hidden, jnp.bfloat16),
            pltpu.SemaphoreType.DMA((2, n_win)),
            pltpu.SemaphoreType.DMA((2,)),
            pltpu.SemaphoreType.DMA((2,)),
            pltpu.SemaphoreType.DMA((tokens // BLOCK,)),
        ],
        compiler_params=pltpu.CompilerParams(vmem_limit_bytes=60 * 2**20),
        cost_estimate=pl.CostEstimate(flops=tokens * n_win * WIN * hidden, bytes_accessed=2 * tokens * hidden, transcendentals=0),
        name="combine",
    )(active, bound, src, *tables, col, gate, *olds)


def solution(mesh):
    tp_size = mesh.shape["tp"]
    ep_size = mesh.shape["ep"]
    assert tp_size == 4

    def whole_moe(act_loc, idx_loc, gate_loc, w_in, w_out):
        tokens, hidden = act_loc.shape
        local_experts = w_in.shape[0]
        assert idx_loc.shape[1] == 1 and local_experts == 2
        experts = local_experts * ep_size
        capacity = capacity_of(1, tokens, experts, tp_size)
        shares = tp_size // local_experts
        chunks = len(SHARES)
        pieces = [capacity // shares * n // sum(SHARES) for n in SHARES]
        heads = [shares * sum(pieces[:q]) for q in range(chunks)]
        assert shares * sum(pieces) == capacity and all(ep_size * p % ROW_TILE == 0 and p % WIN == 0 for p in pieces)
        assert tokens % BLOCK == 0 and BLOCK % LANES == 0
        rank = lax.axis_index("tp")
        which = rank // shares

        twin = [(i, i ^ 1) for i in range(tp_size)]
        mirror = [(i, tp_size - 1 - i) for i in range(tp_size)]
        w_ins, w_outs = [], []
        for whole, kept in ((w_in, w_ins), (w_out, w_outs)):
            mine = lax.dynamic_index_in_dim(whole, which, 0, keepdims=False)
            other = lax.dynamic_index_in_dim(whole, 1 - which, 0, keepdims=False)
            across = lax.ppermute(other, "tp", mirror)
            near = lax.ppermute(mine, "tp", twin)
            far = lax.ppermute(across, "tp", twin)
            kept += [mine, near, across, far]

        blocks = tokens // LANES
        chosen = idx_loc.reshape(blocks, LANES)
        hits = chosen[None] == jnp.arange(experts, dtype=jnp.int32)[:, None, None]
        within = int_dot("ebi,ij->ebj", hits, tri(LANES, True))
        totals = within[:, :, LANES - 1]
        base = int_dot("eb,bc->ec", totals, tri(blocks, False))
        upto = base + totals
        slot = jnp.sum(jnp.where(hits, base[:, :, None] + within - 1, 0.0), axis=0).astype(jnp.int32)

        mine_of = lambda a: lax.dynamic_index_in_dim(a.reshape((ep_size, local_experts) + a.shape[1:]), which, 1, keepdims=False)
        my_within, my_base, my_upto = mine_of(within), mine_of(base), mine_of(upto)
        my_slot = jnp.concatenate([heads[q] + (rank % shares) * pieces[q] + jnp.arange(pieces[q], dtype=jnp.int32) for q in range(chunks)])
        my_slot = my_slot.astype(jnp.float32)
        in_block = jnp.sum((my_upto[:, None, :] <= my_slot[None, :, None]).astype(jnp.int32), axis=2)
        is_block = in_block[:, :, None] == jnp.arange(blocks, dtype=jnp.int32)
        row_within = int_dot("dsb,dbi->dsi", is_block, my_within)
        row_base = jnp.sum(jnp.where(is_block, my_base[:, None, :], 0.0), axis=2)
        in_row = jnp.sum((row_within <= (my_slot[None, :] - row_base)[:, :, None]).astype(jnp.int32), axis=2)
        tok = jnp.where(in_block < blocks, in_block * LANES + in_row, tokens)

        n_win = -(-(BLOCK + experts * 2 * (WIN - 1)) // WIN)
        n_win = -(-n_win * WIN // LANES) * LANES // WIN
        steps = tokens // BLOCK
        first = jnp.minimum(base[:, :: BLOCK // LANES], capacity).astype(jnp.int32).T
        last = jnp.minimum(upto[:, BLOCK // LANES - 1 :: BLOCK // LANES], capacity).astype(jnp.int32).T
        win_lo = first // WIN
        win_hi = jnp.where(last > first, (last - 1) // WIN + 1, win_lo)
        sources = tp_size * ep_size
        mates = [rank ^ x for x in range(tp_size)]
        of_mates = lambda a: jnp.stack([lax.dynamic_index_in_dim(a.reshape(steps, ep_size, local_experts), m // shares, 2, keepdims=False) for m in mates], axis=1).reshape(steps, 1, sources)
        head_w = jnp.asarray([h // WIN for h in heads], jnp.int32)[:, None]
        piece_w = jnp.asarray([p // WIN for p in pieces], jnp.int32)[:, None]
        edge = jnp.repeat(jnp.concatenate([head_w + (m % shares) * piece_w for m in mates], axis=1), ep_size, axis=1)[None]
        lo = jnp.maximum(of_mates(win_lo), edge)
        count = jnp.maximum(jnp.minimum(of_mates(win_hi), edge + piece_w[None]) - lo, 0)
        ends = int_dot("sqe,ef->sqf", count, tri(sources, True)).astype(jnp.int32)
        starts = ends - count
        half = ep_size // 2
        segments = [0, ep_size, 2 * ep_size, 2 * ep_size + half, 3 * ep_size]
        bound = jnp.stack([starts[:, :, at] for at in segments] + [ends[:, :, sources - 1]], axis=2)
        n_fetch = ends[:, :, sources - 1].T
        row_d = jnp.asarray([d - half if x == 2 and d >= half else d for x in range(tp_size) for d in range(ep_size)], jnp.int32)
        w_id = jnp.arange(n_win, dtype=jnp.int32)
        of_source = jnp.sum((ends[:, :, None, :] <= w_id[None, None, :, None]).astype(jnp.int32), axis=3)
        is_source = of_source[:, :, :, None] == jnp.arange(sources, dtype=jnp.int32)
        src = jnp.sum(jnp.where(is_source, (lo - edge - starts + row_d * piece_w)[:, :, None, :], 0), axis=3) + w_id
        src = jnp.where(of_source < sources, src, 0)
        busy = n_fetch > 0
        before = int_dot("qs,st->qt", busy, tri(steps, True)).astype(jnp.int32)
        nth = jnp.arange(steps + 1, dtype=jnp.int32)
        active = jnp.sum((before[:, None, :] <= nth[None, :, None]).astype(jnp.int32), axis=2)
        active = jnp.where(nth[None] == steps, before[:, -1:], active)
        slot_rows, expert_rows = slot.reshape(steps, BLOCK), idx_loc.reshape(steps, BLOCK)
        passed = lambda at: sum((slot_rows >= a).astype(jnp.int32) for a in at)
        chunk_of = passed(heads[1:])
        share_of = passed([h + p for h, p in zip(heads, pieces)]) - chunk_of
        of_rank = (expert_rows % local_experts) * shares + share_of
        pair_of = (chunk_of * tp_size + (of_rank ^ rank)) * ep_size + expert_rows // local_experts
        pairs = chunks * sources
        move = ((starts - lo) * WIN + jnp.arange(chunks, dtype=jnp.int32)[None, :, None] * COL_SPAN).reshape(steps, 1, pairs)
        shift = jnp.sum(jnp.where(pair_of[:, :, None] == jnp.arange(pairs, dtype=jnp.int32), move, 0), axis=2)
        col = jnp.where(slot_rows < capacity, slot_rows + shift, -1).astype(jnp.float32)
        gate = gate_loc.reshape(steps, BLOCK)

        def exchange(rows):
            return lax.all_to_all(rows.reshape(ep_size, -1, hidden), "ep", 0, 0, tiled=True)

        outgoing = []
        for of in ((0, 1), (2, 3, 4)):
            rows = [tok[:, sum(pieces[:q]) : sum(pieces[: q + 1])].reshape(-1) for q in of]
            found = jnp.take(act_loc, jnp.concatenate(rows), axis=0, mode="fill", fill_value=0)
            outgoing += jnp.split(found, [sum(r.size for r in rows[: k + 1]) for k in range(len(rows) - 1)])

        def swap(rows, pairs):
            return lax.ppermute(rows, "tp", pairs)

        arrived = [exchange(outgoing[q]) for q in range(chunks)]
        guides = [(active[q], bound[:, q], src[:, q]) for q in range(chunks)]
        made, returned = [], []
        for q in range(chunks):
            made.append(ffn(arrived[q].reshape(-1, hidden), w_ins, w_outs, made[q - 1 : q] if q else [outgoing[2], col, *sum(guides, ())]))
            returned.append(exchange(made[q]))
        out = None
        tables = []
        for q in range(chunks):
            own = returned[q]
            near, across = swap(own, twin), swap(own, mirror)
            far = [swap(across[:half], twin), swap(near[half:], mirror)]
            tables.append([t.reshape(-1, hidden) for t in (own, near, *far, across)])
        for q in range(chunks):
            out = combine(q, n_win, *guides[q], tables[q], col, gate, out)
        return out

    tok_spec = P(("dp", "ep"), None)


    return jax.shard_map(whole_moe, mesh=mesh, in_specs=(tok_spec, tok_spec, tok_spec, P("ep", None, "tp"), P("ep", "tp", None)), out_specs=tok_spec, check_vma=False)
```
